512 devices in a mesh: orb: 64 (over x, y_hi, z), tm: 8 (over y_lo, core).
Axes of the slice: x: 4, y: 8 (y_hi: 2, y_lo: 4; y = y_hi * 4 + y_lo), z: 8, core: 2. Of those that a mesh axis runs over, the one named last changes fastest.
Arguments:
- integrals: bfloat16 [8192, 128, 128], P('orb'), may hold values from -6 to 6
- block_map: int32 [512, 4], P('orb'), may hold values 0 or 1
- green_occ: bfloat16 [8, 8192, 384], P('tm', 'orb'), may hold values from -0.5 to 0.5
- green_virt: bfloat16 [8, 8192, 384], P('tm', 'orb'), may hold values from -0.5 to 0.5
- coulomb: bfloat16 [8192, 512], P('orb'), may hold values from -0.0048828125 to 0.0048828125
- cosine: float32 [8, 8], replicated, may hold values from -1 to 1
Outputs:
- spectrum: float32 [8, 8192, 512], P('tm', 'orb')
The draws below stay inside these ranges and needn't reach their ends.
All inputs are finite; a program needn't handle non-finite values. No bound on the sum of `block_map` on one device may be relied on, other than what follows from the above.
Results may differ from the reference program's by a relative error of at most 0.0057.
Values may be sent and summed in bfloat16 or wider, within the bound.
No kernel may reach another device: no remote copies, remote signals or barrier semaphores. Data moves between devices by JAX's collectives and lax.ppermute only.
A program may use at most 128 MiB of HBM per device.

```python
import jax
import jax.numpy as jnp
from jax import lax

ORB_DEV = 128
KW = 512
MCOL = 32
BLOCK = 16
AUX_DEV = 128
DOMAINS = 64
NORB = 8192
AUX = 8192
TIMES = 8
FREQS = 8


def place_ends(result, rng, low, largest):
    index_at = [jax.random.randint(jax.random.fold_in(rng, axis), (), 0, length) for axis, length in enumerate(result.shape)]
    main_axis = result.shape.index(max(result.shape))
    beside = index_at[:main_axis] + [(index_at[main_axis] + 1) % result.shape[main_axis]] + index_at[main_axis + 1:]
    return result.at[tuple(index_at)].set(low).at[tuple(beside)].set(largest)


def levels(own_key, shape, pieces, least, high):
    def one(position, blocks):
        heights = jax.random.uniform(jax.random.fold_in(jax.random.fold_in(own_key, 6), position), (blocks,), jnp.float32, least / len(pieces), high / len(pieces))
        return jnp.repeat(jnp.exp(heights), shape[position] // blocks).reshape((-1,) + (1,) * (len(shape) - position - 1))

    gain = one(*pieces[0])
    for cut in pieces[1:]:
        gain = gain * one(*cut)
    return gain


def bell_draw(own_key, extent, deviation, most, pieces=(), held_as=jnp.bfloat16):
    result = deviation * jax.random.normal(own_key, extent, jnp.float32)
    if pieces:
        result = result * levels(own_key, extent, pieces, -0.22, 0.18)
    return jnp.clip(result, -most, most).astype(held_as)


def setup_inputs(seed: int = 0) -> dict:
    keys = jax.random.split(jax.random.key(seed), 7)
    integrals = bell_draw(keys[0], (AUX, ORB_DEV, ORB_DEV), 1.0, 6.0, ((0, 64),))
    block_map = place_ends((jax.random.randint(keys[1], (AUX // BLOCK, ORB_DEV // MCOL), 0, 2) < 1).astype(jnp.int32), jax.random.fold_in(keys[1], 1), 0, 1)
    green_occ = bell_draw(keys[2], (TIMES, NORB, 3 * ORB_DEV), ORB_DEV ** -0.5, 0.5, ((0, 8), (1, 64)))
    green_virt = bell_draw(keys[3], (TIMES, NORB, 3 * ORB_DEV), ORB_DEV ** -0.5, 0.5, ((0, 8), (1, 64)))
    coulomb = bell_draw(keys[4], (AUX, KW), (3 * AUX_DEV * ORB_DEV * ORB_DEV // 4) ** -0.5, 0.0048828125, ((0, 64),))
    cosine = jnp.clip(jax.random.uniform(keys[5], (FREQS, TIMES), jnp.float32, -1.0, 1.0), -1.0, 1.0)
    return {"integrals": integrals, "block_map": block_map, "green_occ": green_occ, "green_virt": green_virt, "coulomb": coulomb, "cosine": cosine}


def reference(integrals, block_map, green_occ, green_virt, coulomb, cosine):
    keep_mask = block_map.astype(jnp.bfloat16)[:, None, :, None, None]
    shaped = integrals.reshape(AUX // BLOCK, BLOCK, ORB_DEV // MCOL, MCOL, ORB_DEV)
    masked = (shaped * keep_mask).reshape(DOMAINS, AUX_DEV, ORB_DEV, ORB_DEV)
    occ_tiles = green_occ.reshape(TIMES, DOMAINS, ORB_DEV, 3, ORB_DEV)
    virt_tiles = green_virt.reshape(TIMES, DOMAINS, ORB_DEV, 3, ORB_DEV)
    coulomb_rows = coulomb.reshape(DOMAINS, AUX_DEV, KW)
    pair_count = ORB_DEV * ORB_DEV

    def one_time(tile_pair):
        occ_time, virt_time = tile_pair

        def one_domain(domain_index):
            own_flat = masked[domain_index].reshape(AUX_DEV, pair_count)
            running_sum = jnp.zeros((AUX_DEV, KW), jnp.float32)
            for offset in range(3):
                neighbor_index = (domain_index + offset - 1) % DOMAINS
                source = masked[neighbor_index].astype(jnp.float32)
                occ_tile = occ_time[domain_index, :, offset, :].astype(jnp.float32)
                virt_tile = virt_time[domain_index, :, offset, :].astype(jnp.float32)
                half_side = jnp.einsum("qls,ns->qln", source, virt_tile).astype(jnp.bfloat16)
                pair_side = jnp.einsum("ml,qln->qmn", occ_tile, half_side.astype(jnp.float32)).astype(jnp.bfloat16)
                response = lax.dot_general(own_flat, pair_side.reshape(AUX_DEV, pair_count), (((1,), (1,)), ((), ())), preferred_element_type=jnp.float32).astype(jnp.bfloat16)
                running_sum = running_sum + jnp.dot(response, coulomb_rows[neighbor_index], preferred_element_type=jnp.float32)
            return running_sum.astype(jnp.bfloat16)

        return lax.map(one_domain, jnp.arange(DOMAINS, dtype=jnp.int32))

    panels = lax.map(one_time, (occ_tiles, virt_tiles)).reshape(TIMES, AUX, KW)
    return jnp.einsum("ft,tpk->fpk", cosine, panels.astype(jnp.float32), precision=lax.Precision.HIGHEST)
```

```python
import functools

import jax
import jax.numpy as jnp
from jax import lax
from jax.experimental import pallas as pl
from jax.experimental.pallas import tpu as pltpu
from jax.sharding import PartitionSpec as P

NT = (((1,), (1,)), ((), ()))
VMEM = pl.BlockSpec(memory_space=pltpu.VMEM)


def flatten_kernel(source, out, wide):
    count, orb, _ = source.shape
    pitch = wide.shape[0] // count
    for p in range(count):
        wide[p * pitch : p * pitch + orb, :] = source[p].astype(jnp.float32)
    for m in range(orb):
        out[:, m * orb : (m + 1) * orb] = wide[pl.ds(m, count, stride=pitch), :].astype(out.dtype)


def flatten(integrals):
    count, orb, _ = integrals.shape
    width = count // 2
    return pl.pallas_call(
        flatten_kernel,
        out_shape=jax.ShapeDtypeStruct((count, orb * orb), integrals.dtype),
        grid=(count // width,),
        in_specs=[pl.BlockSpec((width, orb, orb), lambda i: (i, 0, 0))],
        out_specs=pl.BlockSpec((width, orb * orb), lambda i: (i, 0)),
        scratch_shapes=[pltpu.VMEM((width * (orb + 8), orb), jnp.float32)],
        name="flat",
    )(integrals)


def share_kernel(nq, nt, orb, count, select, *refs):
    sources = refs[:count]
    occ, virt, own_far, keep, weights = refs[count : count + 5]
    outs = refs[count + 5 : 2 * count + 5]
    half, pair, own, arrived = refs[2 * count + 5 :]
    fetch = pltpu.make_async_copy(own_far, own, arrived)
    fetch.start()
    rows = nq * nt * count
    pitch = pair.shape[0] // rows
    group = min(nq, 4)

    for k in range(count):
        lane0 = pl.ds(pl.multiple_of(select[k] * orb, orb), orb)

        def half_step(i, carry):
            tiles = virt[pl.ds(2 * i, 2), :, lane0].reshape(2 * orb, orb)
            for g in range(nq // group):
                left = sources[k][g * group : (g + 1) * group].reshape(group * orb, orb)
                value = lax.dot_general(left, tiles, NT, preferred_element_type=jnp.float32)
                half[g * group : (g + 1) * group, :, pl.ds(pl.multiple_of(2 * i * orb, 2 * orb), 2 * orb)] = (
                    value.astype(jnp.bfloat16).reshape(group, orb, 2 * orb)
                )
            return carry

        lax.fori_loop(0, nt // 2, half_step, 0, unroll=True)

        def pair_step(t, carry):
            tile = occ[t, :, lane0]
            lanes = pl.ds(pl.multiple_of(t * orb, orb), orb)
            for q in range(0, nq, 2):
                right = jnp.concatenate([half[q, :, lanes], half[q + 1, :, lanes]], axis=1)
                value = jnp.dot(tile, right, preferred_element_type=jnp.float32)
                row = pl.multiple_of(((k * nt + t) * nq + q) * pitch, 8)
                pair[pl.ds(row, orb), :] = value[:, :orb]
                pair[pl.ds(row + pitch, orb), :] = value[:, orb:]
            return carry

        lax.fori_loop(0, nt, pair_step, 0, unroll=4)

    fetch.wait()
    blocks = keep.shape[0]
    chunk = orb // blocks

    def response_step(c, total):
        left = jnp.concatenate(
            [pair[pl.ds(c * chunk + i, rows, stride=pitch), :].astype(jnp.bfloat16) for i in range(chunk)],
            axis=1,
        )
        right = own[:, pl.ds(pl.multiple_of(c * chunk * orb, chunk * orb), chunk * orb)]
        value = lax.dot_general(left, right, NT, preferred_element_type=jnp.float32)
        return total + value * keep[c]

    total = lax.fori_loop(0, blocks, response_step, jnp.zeros((rows, own.shape[0]), jnp.float32))
    response = total.astype(jnp.bfloat16)
    for k in range(count):
        piece = response[k * nq * nt : (k + 1) * nq * nt]
        result = jnp.dot(weights[0], piece, preferred_element_type=jnp.float32)
        for i in range(1, weights.shape[0]):
            result += jnp.dot(weights[i], piece, preferred_element_type=jnp.float32)
        outs[k][...] = result.astype(outs[k].dtype)


def share_call(select, sources, occ, virt, own, keep, weights):
    nq, orb, _ = sources[0].shape
    nt = occ.shape[0]
    count = len(sources)
    pitch = orb + 8
    out = jax.ShapeDtypeStruct((weights.shape[1], own.shape[0]), jnp.bfloat16)
    return pl.pallas_call(
        functools.partial(share_kernel, nq, nt, orb, count),
        out_shape=[out] * count,
        in_specs=[pl.BlockSpec(memory_space=pltpu.SMEM)]
        + [VMEM] * (count + 2)
        + [pl.BlockSpec(memory_space=pltpu.HBM)]
        + [VMEM] * 2,
        out_specs=[VMEM] * count,
        scratch_shapes=[
            pltpu.VMEM((nq, orb, nt * orb), jnp.bfloat16),
            pltpu.VMEM((nq * nt * count * pitch, orb), jnp.float32),
            pltpu.VMEM(own.shape, own.dtype),
            pltpu.SemaphoreType.DMA,
        ],
        compiler_params=pltpu.CompilerParams(vmem_limit_bytes=40 * 2**20),
    )(select, *sources, occ, virt, own, keep, weights)


AXES = ("orb", "tm")
SEGMENT = 8


def chain_pairs(domains, groups, first, step):
    pairs = []
    for here in range(first, domains, 2):
        there = (here + step) % domains
        far = here // SEGMENT != there // SEGMENT
        for t in range(groups):
            pairs.append((here * groups + t, there * groups + (mirrored(groups, t) if far else t)))
    return pairs


def mirrored(groups, t):
    return groups - 2 - t + 2 * (t % 2)


def cosine_weights(cosine, nq):
    full = (cosine[:, None, :, None] * jnp.eye(nq, dtype=jnp.float32)[None, :, None, :]).reshape(
        cosine.shape[0] * nq, cosine.shape[1] * nq
    )
    terms = []
    for _ in range(3):
        term = lax.reduce_precision(full, 8, 7)
        terms.append(term.astype(jnp.bfloat16))
        full = full - term
    return jnp.stack(terms)


def tie(value, *others):
    return lax.optimization_barrier((value,) + others)[0]


def body(integrals, block_map, green_occ, green_virt, coulomb, cosine):
    return steps(integrals, block_map, green_occ[0], green_virt[0], coulomb, cosine)


def steps(integrals, block_map, occ_own, virt_own, coulomb, cosine):
    aux_rows, orb, _ = integrals.shape
    row_blocks, col_blocks = block_map.shape
    groups = lax.axis_size("tm")
    domains = lax.axis_size("orb")
    share = aux_rows // groups
    here = lax.axis_index("orb")
    t = lax.axis_index("tm")
    core = t % 2
    odd = here % 2
    place = here % SEGMENT
    far = (place == 0) | (place == SEGMENT - 1)
    map_rows = jnp.repeat(block_map, aux_rows // row_blocks, axis=0)

    def cut(index):
        rows = lax.dynamic_slice_in_dim(integrals, index * share, share, 0)
        mask = lax.dynamic_slice_in_dim(map_rows, index * share, share, 0).astype(jnp.bfloat16)
        return rows * jnp.repeat(mask, orb // col_blocks, axis=1)[:, :, None]

    far_pairs = chain_pairs(domains, groups, 1, 1) + chain_pairs(domains, groups, 0, -1)
    even = chain_pairs(domains, groups, 0, 1) + chain_pairs(domains, groups, 1, -1)
    twin = [(i, i ^ 1) for i in range(groups)]
    far_share = cut(jnp.where(far, mirrored(groups, t), t))
    own_share = cut(tie(t, far_share))
    give = jnp.where(core == 0, virt_own, occ_own)
    kept = jnp.where(core == 0, occ_own, virt_own)
    got = lax.ppermute(give, "tm", twin)
    both = jnp.where(core == 0, jnp.stack([kept, got]), jnp.stack([got, kept]))
    lines = [list(range(c, groups, 2)) for c in range(2)]
    spread = jnp.broadcast_to(both[None], (groups // 2,) + both.shape)
    mine = lax.all_to_all(
        spread, "tm", split_axis=0, concat_axis=0, tiled=True, axis_index_groups=lines
    ).reshape(groups, orb, -1)
    source_b = lax.ppermute(far_share, AXES, far_pairs)
    source_a = lax.ppermute(own_share, AXES, even)
    coulomb_b = lax.ppermute(coulomb, AXES, far_pairs)
    coulomb_a = lax.ppermute(coulomb, AXES, even)
    own = flatten(integrals)
    other = lax.ppermute(mine, "tm", twin)
    occ = jnp.where(core == 0, mine, other)
    virt = jnp.where(core == 0, other, mine)
    keep = jnp.repeat(block_map.T.astype(jnp.float32), aux_rows // row_blocks, axis=1)[:, None, :]
    weights = cosine_weights(cosine, share)
    near = jnp.stack([1 + 0 * odd, 2 - 2 * odd]).astype(jnp.int32)
    part_own, part_a = share_call(near, (own_share, source_a), occ, virt, own, keep, weights)
    (part_b,) = share_call(
        (2 * odd).astype(jnp.int32)[None], (source_b,), occ, virt, own, keep, weights
    )
    mixed = jnp.concatenate([x.reshape(groups, share, aux_rows) for x in (part_own, part_a, part_b)], axis=1)
    mixed = lax.all_to_all(mixed, "tm", split_axis=0, concat_axis=0, tiled=True)
    columns = jnp.concatenate(
        [c.reshape(groups, share, c.shape[1]) for c in (coulomb, coulomb_a, coulomb_b)], axis=1
    )
    return lax.dot_general(
        mixed.reshape(-1, aux_rows),
        columns.reshape(-1, coulomb.shape[1]),
        (((0,), (0,)), ((), ())),
        preferred_element_type=jnp.float32,
    )[None]


def solution(mesh):
    in_specs = (
        P("orb", None, None),
        P("orb", None),
        P("tm", "orb", None),
        P("tm", "orb", None),
        P("orb", None),
        P(),
    )
    out_specs = P("tm", "orb", None)
    return jax.shard_map(body, mesh=mesh, in_specs=in_specs, out_specs=out_specs, check_vma=False)
```

```python
import functools

import jax
import jax.numpy as jnp
from jax import lax
from jax.experimental import pallas as pl
from jax.experimental.pallas import tpu as pltpu
from jax.sharding import PartitionSpec as P

SEGMENT = 8
NT = (((1,), (1,)), ((), ()))
VMEM = pl.BlockSpec(memory_space=pltpu.VMEM)
SMEM = pl.BlockSpec(memory_space=pltpu.SMEM)


def places():
    here, t = lax.axis_index("orb"), lax.axis_index("tm")
    place = lax.rem(here, SEGMENT)
    far = (place == 0) | (place == SEGMENT - 1)
    return lax.rem(here, 2), t, jnp.where(far, mirrored(lax.axis_size("tm"), t), t)


def mirrored(groups, t):
    return groups - 2 - t + 2 * (t % 2)


def prologue_kernel(block_map, integrals, occ, virt, coulomb, spread, own_out, far_out, rows, arrived, copied):
    share, orb, _ = far_out.shape
    place = places()[1:]
    copies = []
    for i in range(own_out.shape[0] - share):
        copies.append(
            pltpu.make_async_copy(coulomb.at[:, i * orb : (i + 1) * orb], own_out.at[share + i], arrived.at[2 + i])
        )
    for i in range(spread.shape[0]):
        for kind, tile in enumerate((occ, virt)):
            copies.append(pltpu.make_async_copy(tile, spread.at[i, kind], copied.at[i, kind]))
    loads = []
    for number in range(2):
        start = pl.multiple_of(place[number] * share, share)
        loads.append(
            pltpu.make_async_copy(integrals.at[pl.ds(start, share)], rows.at[number], arrived.at[number])
        )
    for copy in loads + copies:
        copy.start()
    blocks = block_map.shape[0]
    chunk = orb // blocks
    for number, out in ((1, far_out), (0, own_out)):
        loads[number].wait()
        for j in range(blocks):
            keep = block_map[j, place[number]].astype(jnp.float32)
            part = slice(j * chunk, (j + 1) * chunk)
            out[:share, part, :] = rows[number, :, part, :] * jnp.full((1, 1, orb), keep).astype(out.dtype)
    for copy in copies:
        copy.wait()


def prologue(block_map, integrals, occ, virt, coulomb, copies, share):
    orb = integrals.shape[1]
    lanes = coulomb.shape[1] // orb
    shape = lambda count: jax.ShapeDtypeStruct((count, orb, orb), integrals.dtype)
    return pl.pallas_call(
        prologue_kernel,
        out_shape=[jax.ShapeDtypeStruct((copies, 2) + occ.shape, occ.dtype), shape(share + lanes), shape(share)],
        in_specs=[pl.BlockSpec(memory_space=pltpu.SMEM)] + [pl.BlockSpec(memory_space=pltpu.HBM)] * 4,
        out_specs=[VMEM] * 3,
        scratch_shapes=[
            pltpu.VMEM((2, share, orb, orb), integrals.dtype),
            pltpu.SemaphoreType.DMA((2 + lanes,)),
            pltpu.SemaphoreType.DMA((copies, 2)),
        ],
    )(block_map.T, integrals, occ, virt, coulomb)


def cosine_weights(cosine, nq, nt, kind):
    core = lax.rem(lax.axis_index("tm"), 2)
    core = core if kind == 0 else 1 - core
    freqs = cosine.shape[0]
    row = lax.broadcasted_iota(jnp.int32, (freqs * nq, nt * nq), 0)
    col = lax.broadcasted_iota(jnp.int32, (freqs * nq, nt * nq), 1)
    block = jnp.where(row % nq == col % nq, (row // nq) * nt + col // nq, -1)
    full = jnp.zeros(row.shape, jnp.float32)
    for f in range(freqs):
        for y in range(nt):
            full = jnp.where(block == f * nt + y, cosine[f, 2 * y + core], full)
    terms = []
    for _ in range(3):
        term = full.astype(jnp.bfloat16)
        terms.append(term)
        full = full - term.astype(jnp.float32)
    return terms


def pair_and_respond(nq, jobs, selects, sources, tiles, own_far, block_map, cosine, half, pair, first):
    nt, _, orb, _ = tiles[0].shape
    step_rows = nq * nt
    rows = step_rows * len(jobs)
    pitch = orb + 8
    group = min(nq, 4)
    count = own_far.shape[0]
    if first:
        natural, wide, arrived, own_out = first
        fetch = pltpu.make_async_copy(own_far, natural, arrived)
        fetch.start()
    for number, (k, kind) in enumerate(jobs):
        if number == 1 and first:
            fetch.wait()
        source, tile = sources[k], tiles[kind]
        lane0 = pl.ds(pl.multiple_of(selects[k] * orb, orb), orb)
        for i in range(nt // 2):
            right = tile[2 * i : 2 * i + 2, 1, :, lane0].reshape(2 * orb, orb)
            for g in range(nq // group):
                left = source[g * group : (g + 1) * group].reshape(group * orb, orb)
                value = lax.dot_general(left, right, NT, preferred_element_type=jnp.float32)
                half[g * group : (g + 1) * group, :, 2 * i * orb : 2 * (i + 1) * orb] = (
                    value.astype(jnp.bfloat16).reshape(group, orb, 2 * orb)
                )
        for t in range(nt):
            if number > 0 and first:
                steps = nt * (len(jobs) - 1)
                step = nt * (number - 1) + t
                for p in range(count * step // steps, count * (step + 1) // steps):
                    wide[p * pitch : p * pitch + orb, :] = natural[p].astype(jnp.float32)
            left = tile[t, 0, :, lane0]
            for q in range(0, nq, 2):
                right = jnp.concatenate(
                    [half[q, :, t * orb : (t + 1) * orb], half[q + 1, :, t * orb : (t + 1) * orb]], axis=1
                )
                value = jnp.dot(left, right, preferred_element_type=jnp.float32)
                row = (number * step_rows + t * nq + q) * pitch
                pair[row : row + orb, :] = value[:, :orb]
                pair[row + pitch : row + pitch + orb, :] = value[:, orb:]
    blocks, row_blocks = block_map.shape
    chunk = orb // blocks
    column = lax.broadcasted_iota(jnp.int32, (1, count), 1) // (count // row_blocks)

    def response_step(c, total):
        left = jnp.concatenate(
            [pair[pl.ds(c * chunk + i, rows, stride=pitch), :].astype(jnp.bfloat16) for i in range(chunk)],
            axis=1,
        )
        lanes = pl.ds(pl.multiple_of(c * chunk * orb, chunk * orb), chunk * orb)
        if first:
            right = jnp.concatenate(
                [wide[pl.ds(c * chunk + i, count, stride=pitch), :].astype(jnp.bfloat16) for i in range(chunk)],
                axis=1,
            )
            own_out[:, lanes] = right
        else:
            right = own_far[:, lanes]
        value = lax.dot_general(left, right, NT, preferred_element_type=jnp.float32)
        keep = jnp.zeros((1, count), jnp.float32)
        for b in range(row_blocks):
            keep = jnp.where(column == b, block_map[c, b].astype(jnp.float32), keep)
        return total + value * keep

    total = lax.fori_loop(0, blocks, response_step, jnp.zeros((rows, count), jnp.float32))
    response = total.astype(jnp.bfloat16)
    weights = [cosine_weights(cosine, nq, nt, kind) for kind in range(len(tiles))]
    sums = [None] * len(sources)
    for number, (k, kind) in enumerate(jobs):
        piece = response[number * step_rows : (number + 1) * step_rows]
        for weight in weights[kind]:
            term = jnp.dot(weight, piece, preferred_element_type=jnp.float32)
            sums[k] = term if sums[k] is None else sums[k] + term
    return sums


def near_kernel(nq, own_share, beside, mine, other, integrals, block_map, cosine, out, own_out, half, pair, natural, wide, arrived):
    odd = lax.rem(lax.axis_index("orb"), 2)
    jobs = ((0, 0), (1, 0), (0, 1), (1, 1))
    sums = pair_and_respond(
        nq, jobs, (1, 2 - 2 * odd), (own_share, beside), (mine, other), integrals, block_map, cosine, half, pair,
        (natural, wide, arrived, own_out),
    )
    for k, value in enumerate(sums):
        out[k] = value


def below_kernel(nq, source, mine, other, own, block_map, cosine, out, half, pair):
    odd = lax.rem(lax.axis_index("orb"), 2)

    @pl.when(odd == 0)
    def _():
        jobs = ((0, 0), (0, 1))
        out[...] = pair_and_respond(
            nq, jobs, (0,), (source,), (mine, other), own, block_map, cosine, half, pair, None
        )[0]


def above_kernel(nq, source, mine, other, own, block_map, cosine, near, below, out, half, pair):
    odd = lax.rem(lax.axis_index("orb"), 2)

    def put(k, value):
        out[:, k * nq : (k + 1) * nq, :] = value.astype(out.dtype).reshape(-1, nq, value.shape[1])

    for k in range(near.shape[0]):
        put(k, near[k])

    @pl.when(odd == 0)
    def _():
        put(near.shape[0], below[...])

    @pl.when(odd == 1)
    def _():
        jobs = ((0, 0), (0, 1))
        value = pair_and_respond(
            nq, jobs, (2,), (source,), (mine, other), own, block_map, cosine, half, pair, None
        )
        put(near.shape[0], value[0])


def scratch(nq, tile, jobs):
    nt, _, orb, _ = tile.shape
    return [
        pltpu.VMEM((nq, orb, nt * orb), jnp.bfloat16),
        pltpu.VMEM((nq * nt * jobs * (orb + 8), orb), jnp.float32),
    ]


def near_call(nq, own_share, beside, mine, other, integrals, block_map, cosine):
    count, orb, _ = integrals.shape
    return pl.pallas_call(
        functools.partial(near_kernel, nq),
        out_shape=[
            jax.ShapeDtypeStruct((2, cosine.shape[0] * nq, count), jnp.float32),
            jax.ShapeDtypeStruct((count, orb * orb), integrals.dtype),
        ],
        in_specs=[VMEM] * 4 + [pl.BlockSpec(memory_space=pltpu.HBM)] + [SMEM] * 2,
        out_specs=[VMEM] * 2,
        scratch_shapes=scratch(nq, mine, 4)
        + [
            pltpu.VMEM(integrals.shape, integrals.dtype),
            pltpu.VMEM((count * (orb + 8), orb), jnp.float32),
            pltpu.SemaphoreType.DMA,
        ],
        compiler_params=pltpu.CompilerParams(vmem_limit_bytes=46 * 2**20),
    )(own_share, beside, mine, other, integrals, block_map.T, cosine)


def far_call(nq, source, mine, other, own, block_map, cosine, near=None, below=None):
    last = near is not None
    freqs, count = cosine.shape[0], own.shape[0]
    if last:
        out = jax.ShapeDtypeStruct((freqs, nq * (1 + near.shape[0]), count), jnp.bfloat16)
    else:
        out = jax.ShapeDtypeStruct((freqs * nq, count), jnp.float32)
    return pl.pallas_call(
        functools.partial(above_kernel if last else below_kernel, nq),
        out_shape=out,
        in_specs=[VMEM] * 4 + [SMEM] * 2 + [VMEM] * (2 if last else 0),
        out_specs=VMEM,
        scratch_shapes=scratch(nq, mine, 2),
        compiler_params=pltpu.CompilerParams(vmem_limit_bytes=20 * 2**20),
    )(source, mine, other, own, block_map.T, cosine, *((near, below) if last else ()))


AXES = ("orb", "tm")


def chain_pairs(domains, groups, first, step):
    pairs = []
    for here in range(first, domains, 2):
        there = (here + step) % domains
        far = here // SEGMENT != there // SEGMENT
        for t in range(groups):
            pairs.append((here * groups + t, there * groups + (mirrored(groups, t) if far else t)))
    return pairs


def body(integrals, block_map, green_occ, green_virt, coulomb, cosine):
    return steps(integrals, block_map, green_occ[0], green_virt[0], coulomb, cosine)


def steps(integrals, block_map, occ_own, virt_own, coulomb, cosine):
    aux_rows, _, _ = integrals.shape
    groups = lax.axis_size("tm")
    domains = lax.axis_size("orb")
    share = aux_rows // groups
    up = chain_pairs(domains, groups, 1, 1)
    down = chain_pairs(domains, groups, 0, -1)
    even = chain_pairs(domains, groups, 0, 1) + chain_pairs(domains, groups, 1, -1)
    twin = [(i, i ^ 1) for i in range(groups)]
    lines = [list(range(c, groups, 2)) for c in range(2)]
    spread, own_share, far_share = prologue(
        block_map, integrals, occ_own, virt_own, coulomb, groups // 2, share
    )
    from_below = lax.ppermute(far_share, AXES, up)
    mine = lax.all_to_all(spread, "tm", split_axis=0, concat_axis=0, tiled=True, axis_index_groups=lines)
    source_a = lax.ppermute(own_share, AXES, even)
    from_above = lax.ppermute(far_share, AXES, down)
    coulomb_b = lax.ppermute(coulomb, AXES, up + down)
    coulomb_a = source_a[share:].transpose(1, 0, 2).reshape(aux_rows, -1)
    other = lax.ppermute(mine, "tm", twin)
    near, own = near_call(share, own_share, source_a, mine, other, integrals, block_map, cosine)
    below = far_call(share, from_below, mine, other, own, block_map, cosine)
    mixed = far_call(share, from_above, mine, other, own, block_map, cosine, near, below)
    mixed = lax.all_to_all(mixed, "tm", split_axis=0, concat_axis=0, tiled=True)
    columns = jnp.concatenate(
        [c.reshape(groups, share, c.shape[1]) for c in (coulomb, coulomb_a, coulomb_b)], axis=1
    )
    columns = lax.optimization_barrier(columns)
    return lax.dot_general(
        mixed.reshape(-1, aux_rows),
        columns.reshape(-1, coulomb.shape[1]),
        (((0,), (0,)), ((), ())),
        preferred_element_type=jnp.float32,
    )[None]


def solution(mesh):
    in_specs = (
        P("orb", None, None),
        P("orb", None),
        P("tm", "orb", None),
        P("tm", "orb", None),
        P("orb", None),
        P(),
    )
    out_specs = P("tm", "orb", None)
    return jax.shard_map(body, mesh=mesh, in_specs=in_specs, out_specs=out_specs, check_vma=False)
```

```python
import functools

import jax
import jax.numpy as jnp
from jax import lax
from jax.experimental import pallas as pl
from jax.experimental.pallas import tpu as pltpu
from jax.sharding import PartitionSpec as P

SEGMENT = 8
NT = (((1,), (1,)), ((), ()))
VMEM = pl.BlockSpec(memory_space=pltpu.VMEM)
SMEM = pl.BlockSpec(memory_space=pltpu.SMEM)


def places():
    here, t = lax.axis_index("orb"), lax.axis_index("tm")
    place = lax.rem(here, SEGMENT)
    far = (place == 0) | (place == SEGMENT - 1)
    return lax.rem(here, 2), t, jnp.where(far, mirrored(lax.axis_size("tm"), t), t)


def mirrored(groups, t):
    return groups - 2 - t + 2 * (t % 2)


def prologue_kernel(block_map, integrals, occ, virt, coulomb, spread, own_out, far_out, tiles, rows, arrived, copied):
    share, orb, _ = far_out.shape
    place = places()[1:]
    lanes = own_out.shape[0] - share
    loads = [
        pltpu.make_async_copy(occ, tiles.at[0], arrived.at[0]),
        pltpu.make_async_copy(virt, tiles.at[1], arrived.at[1]),
    ]
    for number in range(2):
        start = pl.multiple_of(place[number] * share, share)
        loads.append(
            pltpu.make_async_copy(
                integrals.at[pl.ds(start, share)], rows.at[number, pl.ds(0, share)], arrived.at[2 + number]
            )
        )
    for i in range(lanes):
        loads.append(
            pltpu.make_async_copy(
                coulomb.at[:, i * orb : (i + 1) * orb], rows.at[0, share + i], arrived.at[4 + i]
            )
        )
    stores = [pltpu.make_async_copy(tiles, spread.at[i], copied.at[i]) for i in range(spread.shape[0])]
    stores.append(pltpu.make_async_copy(rows.at[1, pl.ds(0, share)], far_out, copied.at[len(stores)]))
    stores.append(pltpu.make_async_copy(rows.at[0], own_out, copied.at[len(stores)]))
    for copy in loads:
        copy.start()
    for copy in loads[:2]:
        copy.wait()
    for copy in stores[:-2]:
        copy.start()
    blocks = block_map.shape[0]
    chunk = orb // blocks
    for number in (1, 0):
        loads[2 + number].wait()
        for j in range(blocks):
            keep = block_map[j, place[number]].astype(jnp.float32)
            part = slice(j * chunk, (j + 1) * chunk)
            rows[number, :share, part, :] = rows[number, :share, part, :] * jnp.full((1, 1, orb), keep).astype(rows.dtype)
        if number == 0:
            for copy in loads[4:]:
                copy.wait()
        stores[-1 - number].start()
    for copy in stores:
        copy.wait()


def prologue(block_map, integrals, occ, virt, coulomb, copies, share):
    orb = integrals.shape[1]
    lanes = coulomb.shape[1] // orb
    shape = lambda count: jax.ShapeDtypeStruct((count, orb, orb), integrals.dtype)
    far = pl.BlockSpec(memory_space=pltpu.HBM)
    return pl.pallas_call(
        prologue_kernel,
        out_shape=[jax.ShapeDtypeStruct((copies, 2) + occ.shape, occ.dtype), shape(share + lanes), shape(share)],
        in_specs=[SMEM] + [far] * 4,
        out_specs=[far] * 3,
        scratch_shapes=[
            pltpu.VMEM((2,) + occ.shape, occ.dtype),
            pltpu.VMEM((2, share + lanes, orb, orb), integrals.dtype),
            pltpu.SemaphoreType.DMA((4 + lanes,)),
            pltpu.SemaphoreType.DMA((copies + 2,)),
        ],
    )(block_map.T, integrals, occ, virt, coulomb)


def cosine_weights(cosine, nq, nt, kind):
    core = lax.rem(lax.axis_index("tm"), 2)
    core = core if kind == 0 else 1 - core
    freqs = cosine.shape[0]
    row = lax.broadcasted_iota(jnp.int32, (freqs * nq, nt * nq), 0)
    col = lax.broadcasted_iota(jnp.int32, (freqs * nq, nt * nq), 1)
    block = jnp.where(row % nq == col % nq, (row // nq) * nt + col // nq, -1)
    full = jnp.zeros(row.shape, jnp.float32)
    for f in range(freqs):
        for y in range(nt):
            full = jnp.where(block == f * nt + y, cosine[f, 2 * y + core], full)
    terms = []
    for _ in range(3):
        term = full.astype(jnp.bfloat16)
        terms.append(term)
        full = full - term.astype(jnp.float32)
    return terms


def pair_and_respond(nq, jobs, selects, sources, tiles, own_far, block_map, cosine, half, pair, mixing, first):
    for kind in range(len(tiles)):
        for i, term in enumerate(cosine_weights(cosine, nq, tiles[0].shape[0], kind)):
            mixing[kind, i] = term
    nt, _, orb, _ = tiles[0].shape
    step_rows = nq * nt
    rows = step_rows * len(jobs)
    pitch = orb + 8
    group = min(nq, 8)
    count = own_far.shape[0]
    if first:
        natural, wide, arrived, own_out = first
        fetch = pltpu.make_async_copy(own_far, natural, arrived)
        fetch.start()
    for number, (k, kind) in enumerate(jobs):
        if number == 1 and first:
            fetch.wait()
        source, tile = sources[k], tiles[kind]
        if source is None:
            me = lax.axis_index("tm")
            line = lax.broadcasted_iota(jnp.int32, (1, orb, orb), 1) // (orb // block_map.shape[0])
            mask = jnp.zeros((1, orb, orb), jnp.float32)
            for j in range(block_map.shape[0]):
                mask = jnp.where(line == j, block_map[j, me].astype(jnp.float32), mask)
            mask = mask.astype(jnp.bfloat16)
        lane0 = pl.ds(pl.multiple_of(selects[k] * orb, orb), orb)
        for i in range(nt // 2):
            right = tile[2 * i : 2 * i + 2, 1, :, lane0].reshape(2 * orb, orb)
            for g in range(nq // group):
                if source is None:
                    left = natural[pl.ds(me * nq + g * group, group)] * mask
                else:
                    left = source[g * group : (g + 1) * group]
                left = left.reshape(group * orb, orb)
                value = lax.dot_general(left, right, NT, preferred_element_type=jnp.float32)
                half[g * group : (g + 1) * group, :, 2 * i * orb : 2 * (i + 1) * orb] = (
                    value.astype(jnp.bfloat16).reshape(group, orb, 2 * orb)
                )
        for t in range(nt):
            if number > 0 and first:
                steps = nt * (len(jobs) - 1)
                step = nt * (number - 1) + t
                for p in range(count * step // steps, count * (step + 1) // steps):
                    wide[p * pitch : p * pitch + orb, :] = natural[p].astype(jnp.float32)
            left = tile[t, 0, :, lane0]
            for q in range(0, nq, 2):
                right = jnp.concatenate(
                    [half[q, :, t * orb : (t + 1) * orb], half[q + 1, :, t * orb : (t + 1) * orb]], axis=1
                )
                value = jnp.dot(left, right, preferred_element_type=jnp.float32)
                row = (number * step_rows + t * nq + q) * pitch
                pair[row : row + orb, :] = value[:, :orb]
                pair[row + pitch : row + pitch + orb, :] = value[:, orb:]
    blocks, row_blocks = block_map.shape
    chunk = orb // blocks
    column = lax.broadcasted_iota(jnp.int32, (1, count), 1) // (count // row_blocks)

    def response_step(c, total):
        left = jnp.concatenate(
            [pair[pl.ds(c * chunk + i, rows, stride=pitch), :].astype(jnp.bfloat16) for i in range(chunk)],
            axis=1,
        )
        lanes = pl.ds(pl.multiple_of(c * chunk * orb, chunk * orb), chunk * orb)
        if first:
            right = jnp.concatenate(
                [wide[pl.ds(c * chunk + i, count, stride=pitch), :].astype(jnp.bfloat16) for i in range(chunk)],
                axis=1,
            )
            own_out[:, lanes] = right
        else:
            right = own_far[:, lanes]
        value = lax.dot_general(left, right, NT, preferred_element_type=jnp.float32)
        keep = jnp.zeros((1, count), jnp.float32)
        for b in range(row_blocks):
            keep = jnp.where(column == b, block_map[c, b].astype(jnp.float32), keep)
        return total + value * keep

    total = lax.fori_loop(0, blocks, response_step, jnp.zeros((rows, count), jnp.float32), unroll=4)
    response = total.astype(jnp.bfloat16)
    sums = [None] * len(sources)
    for number, (k, kind) in enumerate(jobs):
        piece = response[number * step_rows : (number + 1) * step_rows]
        for i in range(mixing.shape[1]):
            term = jnp.dot(mixing[kind, i], piece, preferred_element_type=jnp.float32)
            sums[k] = term if sums[k] is None else sums[k] + term
    return sums


def near_kernel(nq, beside, mine, other, integrals, block_map, cosine, out, own_out, half, pair, mixing, natural, wide, arrived):
    odd = lax.rem(lax.axis_index("orb"), 2)
    jobs = ((1, 0), (0, 0), (1, 1), (0, 1))
    sums = pair_and_respond(
        nq, jobs, (1, 2 - 2 * odd), (None, beside), (mine, other), integrals, block_map, cosine, half, pair, mixing,
        (natural, wide, arrived, own_out),
    )
    for k, value in enumerate(sums):
        out[k] = value


def below_kernel(nq, source, mine, other, own, block_map, cosine, out, half, pair, mixing):
    odd = lax.rem(lax.axis_index("orb"), 2)

    @pl.when(odd == 0)
    def _():
        jobs = ((0, 0), (0, 1))
        out[...] = pair_and_respond(
            nq, jobs, (0,), (source,), (mine, other), own, block_map, cosine, half, pair, mixing, None
        )[0]


def above_kernel(nq, source, mine, other, own, block_map, cosine, near, below, out, half, pair, mixing):
    odd = lax.rem(lax.axis_index("orb"), 2)

    def put(k, value):
        out[:, k * nq : (k + 1) * nq, :] = value.astype(out.dtype).reshape(-1, nq, value.shape[1])

    for k in range(near.shape[0]):
        put(k, near[k])

    @pl.when(odd == 0)
    def _():
        put(near.shape[0], below[...])

    @pl.when(odd == 1)
    def _():
        jobs = ((0, 0), (0, 1))
        value = pair_and_respond(
            nq, jobs, (2,), (source,), (mine, other), own, block_map, cosine, half, pair, mixing, None
        )
        put(near.shape[0], value[0])


def scratch(nq, tile, jobs, freqs):
    nt, _, orb, _ = tile.shape
    return [
        pltpu.VMEM((nq, orb, nt * orb), jnp.bfloat16),
        pltpu.VMEM((nq * nt * jobs * (orb + 8), orb), jnp.float32),
        pltpu.VMEM((2, 3, freqs * nq, nt * nq), jnp.bfloat16),
    ]


def near_call(nq, beside, mine, other, integrals, block_map, cosine):
    count, orb, _ = integrals.shape
    return pl.pallas_call(
        functools.partial(near_kernel, nq),
        out_shape=[
            jax.ShapeDtypeStruct((2, cosine.shape[0] * nq, count), jnp.float32),
            jax.ShapeDtypeStruct((count, orb * orb), integrals.dtype),
        ],
        in_specs=[VMEM] * 3 + [pl.BlockSpec(memory_space=pltpu.HBM)] + [SMEM] * 2,
        out_specs=[VMEM] * 2,
        scratch_shapes=scratch(nq, mine, 4, cosine.shape[0])
        + [
            pltpu.VMEM(integrals.shape, integrals.dtype),
            pltpu.VMEM((count * (orb + 8), orb), jnp.float32),
            pltpu.SemaphoreType.DMA,
        ],
        compiler_params=pltpu.CompilerParams(vmem_limit_bytes=46 * 2**20),
    )(beside, mine, other, integrals, block_map.T, cosine)


def far_call(nq, source, mine, other, own, block_map, cosine, near=None, below=None):
    last = near is not None
    freqs, count = cosine.shape[0], own.shape[0]
    if last:
        out = jax.ShapeDtypeStruct((freqs, nq * (1 + near.shape[0]), count), jnp.bfloat16)
    else:
        out = jax.ShapeDtypeStruct((freqs * nq, count), jnp.float32)
    return pl.pallas_call(
        functools.partial(above_kernel if last else below_kernel, nq),
        out_shape=out,
        in_specs=[VMEM] * 4 + [SMEM] * 2 + [VMEM] * (2 if last else 0),
        out_specs=VMEM,
        scratch_shapes=scratch(nq, mine, 2, freqs),
        compiler_params=pltpu.CompilerParams(vmem_limit_bytes=20 * 2**20),
    )(source, mine, other, own, block_map.T, cosine, *((near, below) if last else ()))


AXES = ("orb", "tm")


def chain_pairs(domains, groups, first, step):
    pairs = []
    for here in range(first, domains, 2):
        there = (here + step) % domains
        far = here // SEGMENT != there // SEGMENT
        for t in range(groups):
            pairs.append((here * groups + t, there * groups + (mirrored(groups, t) if far else t)))
    return pairs


def body(integrals, block_map, green_occ, green_virt, coulomb, cosine):
    return steps(integrals, block_map, green_occ[0], green_virt[0], coulomb, cosine)


def steps(integrals, block_map, occ_own, virt_own, coulomb, cosine):
    aux_rows, _, _ = integrals.shape
    groups = lax.axis_size("tm")
    domains = lax.axis_size("orb")
    share = aux_rows // groups
    up = chain_pairs(domains, groups, 1, 1)
    down = chain_pairs(domains, groups, 0, -1)
    even = chain_pairs(domains, groups, 0, 1) + chain_pairs(domains, groups, 1, -1)
    twin = [(i, i ^ 1) for i in range(groups)]
    lines = [list(range(c, groups, 2)) for c in range(2)]
    spread, own_share, far_share = prologue(
        block_map, integrals, occ_own, virt_own, coulomb, groups // 2, share
    )
    from_below = lax.ppermute(far_share, AXES, up)
    mine = lax.all_to_all(spread, "tm", split_axis=0, concat_axis=0, tiled=True, axis_index_groups=lines)
    source_a = lax.ppermute(own_share, AXES, even)
    from_above = lax.ppermute(far_share, AXES, down)
    coulomb_b = lax.ppermute(coulomb, AXES, up + down)
    coulomb_a = source_a[share:].transpose(1, 0, 2).reshape(aux_rows, -1)
    other = lax.ppermute(mine, "tm", twin)
    near, own = near_call(share, source_a, mine, other, integrals, block_map, cosine)
    below = far_call(share, from_below, mine, other, own, block_map, cosine)
    mixed = far_call(share, from_above, mine, other, own, block_map, cosine, near, below)
    mixed = lax.all_to_all(mixed, "tm", split_axis=0, concat_axis=0, tiled=True)
    columns = jnp.concatenate(
        [c.reshape(groups, share, c.shape[1]) for c in (coulomb, coulomb_a, coulomb_b)], axis=1
    )
    columns = lax.optimization_barrier(columns)
    return lax.dot_general(
        mixed.reshape(-1, aux_rows),
        columns.reshape(-1, coulomb.shape[1]),
        (((0,), (0,)), ((), ())),
        preferred_element_type=jnp.float32,
    )[None]


def solution(mesh):
    in_specs = (
        P("orb", None, None),
        P("orb", None),
        P("tm", "orb", None),
        P("tm", "orb", None),
        P("orb", None),
        P(),
    )
    out_specs = P("tm", "orb", None)
    return jax.shard_map(body, mesh=mesh, in_specs=in_specs, out_specs=out_specs, check_vma=False)
```
